32 devices in a mesh: tm: 16 (over z, x, core), chan: 2 (over y).
Axes of the slice: x: 2, y: 2, z: 4, core: 2. Of those that a mesh axis runs over, the one named last changes fastest.
Arguments:
- random_forcing: bfloat16 [6144, 4096], P('tm', 'chan'), may hold values from -6 to 6
- eigen_root_table: float32 [768, 4096], P(None, 'chan'), may hold values from 0.1 to 2
- lane_fading_speed: float32 [4096], P('chan'), may hold values from 3.2552083e-07 to 0.025, as said below
- sudden_shrink: float32 [6144], P('tm'), may hold values from 0.125 to 1, as said below
Outputs:
- sample: float32 [6144, 4096], P('tm', 'chan')
The draws below stay inside these ranges and needn't reach their ends.
Inputs may be any that keep to these rules, and one draw needn't show every extreme that they name: `lane_fading_speed`: every channel's rate is positive. `sudden_shrink`: every entry lies in (0, 1], and the product of all entries is at most 0.52.
All inputs are finite; a program needn't handle non-finite values.
Results may differ from the reference program's by a relative error of at most 0.0003.
Values may be sent and summed in bfloat16 or wider, within the bound.
No kernel may reach another device: no remote copies, remote signals or barrier semaphores. Data moves between devices by JAX's collectives and lax.ppermute only.
A program may use at most 192 MiB of HBM per device.

```python
import math
import jax
import jax.numpy as jnp
from jax import lax

CHANNELS = 4096
BLOCK_TICKS = 384
TIME = 6144
N_TM = 16


def draw_lane_fading_speed(key, part):
    first = jax.random.fold_in(key, 0)
    lowest = 0.002 / TIME
    return jnp.exp(jnp.log(lowest) + jax.random.uniform(first, (CHANNELS,), jnp.float32) * jnp.log(0.025 / lowest)).astype(jnp.float32)


def draw_sudden_shrink(key, part):
    first, second = jax.random.split(jax.random.fold_in(key, 17), 2)
    places = jax.random.permutation(first, TIME)[:3].astype(jnp.int32)
    factors = jax.random.uniform(second, (3,), jnp.float32, 0.5, 0.8)
    positions = jnp.arange(TIME, dtype=jnp.int32)
    scaled = jnp.where(positions[None, :] == places[:, None], factors[:, None], 1.0)
    return jnp.prod(scaled, axis=0).astype(jnp.float32)


def steps_of(key, shape, cuts, least, high):
    def one(axis_at, shards_of):
        heights = jax.random.uniform(jax.random.fold_in(jax.random.fold_in(key, 6), axis_at), (shards_of,), jnp.float32, least / len(cuts), high / len(cuts))
        return jnp.repeat(jnp.exp(heights), shape[axis_at] // shards_of).reshape((-1,) + (1,) * (len(shape) - axis_at - 1))

    loudness = one(*cuts[0])
    for cut in cuts[1:]:
        loudness = loudness * one(*cut)
    return loudness


def noise(key, shape, spread, bound, cuts=(), kind=jnp.bfloat16):
    gain = steps_of(key, shape, cuts, -0.22, 0.18) if cuts else 1.0
    drawn = jax.random.normal(key, shape, jnp.float32) * spread * gain
    return jnp.minimum(jnp.maximum(drawn, -bound), bound).astype(kind)


def setup_inputs(seed: int = 0) -> dict:
    key_of = jax.random.split(jax.random.key(seed), 5)
    random_forcing = noise(key_of[0], (TIME, CHANNELS), 1.0, 6.0, ((0, 16), (1, 2)))
    eigen_root_table = jnp.clip(jnp.exp(math.log(2.0) - 2.9957323 * jax.random.uniform(key_of[1], (2 * BLOCK_TICKS, CHANNELS), jnp.float32) ** steps_of(key_of[1], (2 * BLOCK_TICKS, CHANNELS), ((1, 2),), -0.2, 0.2)), 0.1, 2.0)
    lane_fading_speed = draw_lane_fading_speed(jax.random.fold_in(key_of[4], 71), 0)
    sudden_shrink = draw_sudden_shrink(jax.random.fold_in(key_of[4], 71), 0)
    return {"random_forcing": random_forcing, "eigen_root_table": eigen_root_table, "lane_fading_speed": lane_fading_speed, "sudden_shrink": sudden_shrink}


def combine(former, latter):
    return (former[0] + latter[0], jnp.exp(latter[0]) * former[1] + latter[1])

def reference(random_forcing, eigen_root_table, lane_fading_speed, sudden_shrink):
    sections = random_forcing.astype(jnp.float32).reshape(N_TM, BLOCK_TICKS, CHANNELS)

    def convolve(section):
        padded = jnp.concatenate([section, jnp.zeros_like(section)], axis=0)
        spectra = jnp.fft.fft(padded, axis=0)
        return jnp.real(jnp.fft.ifft(spectra * eigen_root_table, axis=0)).astype(jnp.float32)
    last_trailing = convolve(sections[N_TM - 1])[BLOCK_TICKS:]

    def conv_step(trailing, section):
        entire = convolve(section)
        return (entire[BLOCK_TICKS:], entire[:BLOCK_TICKS] + trailing)
    unused, noise_sequence = lax.scan(conv_step, last_trailing, sections)
    forcing_kicks = sudden_shrink.reshape(N_TM, BLOCK_TICKS)

    def local_scan(paired):
        section, factors = paired
        tick_log_growth = jnp.log(factors)[:, None] - lane_fading_speed[None, :]
        power_entries = (factors * factors)[:, None]
        weights = jnp.sqrt(1.0 - power_entries + power_entries * (-jnp.expm1(-2.0 * lane_fading_speed))[None, :])
        return lax.associative_scan(combine, (tick_log_growth, weights * section), axis=0)

    def section_sums(paired):
        logs, states = local_scan(paired)
        return (logs[-1], states[-1])
    section_logarithm_sum, section_final_state = lax.map(section_sums, (noise_sequence, forcing_kicks))

    def prefix(carried, item):
        return (combine(carried, item), carried)
    zeroes = jnp.zeros((CHANNELS,), jnp.float32)
    entire_total, preceding_input = lax.scan(prefix, (zeroes, zeroes), (section_logarithm_sum, section_final_state))
    opening = entire_total[1] / -jnp.expm1(entire_total[0])

    def section_output(packed):
        paired, before_log, before_state = packed
        logs, states = local_scan(paired)
        incoming = jnp.exp(before_log) * opening + before_state
        return states + jnp.exp(logs) * incoming[None, :]
    field_output = lax.map(section_output, ((noise_sequence, forcing_kicks), preceding_input[0], preceding_input[1]))
    return field_output.reshape(TIME, CHANNELS)
```

```python
import functools

import jax
import jax.numpy as jnp
import numpy as np
from jax import lax
from jax.experimental import pallas as pl
from jax.experimental.pallas import tpu as pltpu
from jax.sharding import PartitionSpec as P

LANES = 128
SEGMENTS = 8
BLOCK = 512
NYQUIST_ROWS = 16


def split(table):
    high = table.astype(jnp.bfloat16)
    low = (table - high.astype(np.float64)).astype(jnp.bfloat16)
    return high, low


def tripled(table):
    high, low = split(table)
    return np.concatenate([high, high, low], axis=1)


def tables(length):
    full = 2 * length
    half = length // 2
    frequency = 2 * np.arange(half)[:, None]
    nyquist = np.full((1, 1), length)

    def angle(frequencies, times):
        return (frequencies * times[None, :] % full) * (2.0 * np.pi / full)

    def parts(times):
        blank = np.zeros((NYQUIST_ROWS - 1, times.size))
        return (
            np.concatenate([np.cos(angle(frequency, times)), np.cos(angle(nyquist, times)), blank]),
            np.sin(angle(frequency, times)),
            np.cos(angle(frequency + 1, times)),
            np.sin(angle(frequency + 1, times)),
        )

    forward = np.concatenate(split(np.concatenate(parts(np.arange(length)))), axis=1)
    ticks = np.arange(length)
    counted = np.where(ticks < half, ticks, length - 1 - ticks)
    segment = half // SEGMENTS
    times = (np.arange(segment + 1)[:, None] + segment * np.arange(SEGMENTS)[None, :]).reshape(-1)
    even_cos, even_sin, odd_cos, odd_sin = (tripled(part.T / full) for part in parts(times))
    sums = np.concatenate([even_cos, odd_sin], axis=1)
    differences = np.concatenate([even_sin, odd_cos], axis=1)
    rows = counted // segment == np.arange(SEGMENTS)[:, None]
    blocks = counted % segment + np.where(ticks < half, 0, segment)
    blocks = blocks[:, None] == np.arange(2 * segment)
    return (
        forward, even_cos, even_sin, odd_cos, odd_sin, sums, differences,
        rows.astype(np.float32), blocks.astype(np.float32),
    )


def dot(left, right):
    return jnp.dot(left, right, preferred_element_type=jnp.float32)


def stacked(values):
    high = values.astype(jnp.bfloat16)
    low = (values - high.astype(jnp.float32)).astype(jnp.bfloat16)
    return jnp.concatenate([high, low, high], axis=0)


def spectra(section, evens, nyquist, odds, forward_ref):
    half = section.shape[0] // 2
    doubled = jnp.concatenate([section, section], axis=0)
    first = half + NYQUIST_ROWS
    scale = jnp.concatenate(
        [evens, jnp.broadcast_to(nyquist, (NYQUIST_ROWS, evens.shape[1]))], axis=0
    )
    even_cos = stacked(dot(forward_ref[:first], doubled) * scale)
    starts = (first, first + half, first + 2 * half)
    even_sin, odd_cos, odd_sin = (
        stacked(dot(forward_ref[at : at + half], doubled) * scale)
        for at, scale in zip(starts, (evens, odds, odds))
    )
    return even_cos, even_sin, odd_cos, odd_sin


def turned(x):
    row = lax.broadcasted_iota(jnp.int32, x.shape, 0)
    return jnp.take_along_axis(x, SEGMENTS - 1 - row, axis=0, mode="promise_in_bounds")


def mirrored(table_ref):
    full = table_ref.shape[0]
    half = full // 4
    row = lax.broadcasted_iota(jnp.int32, (SEGMENTS, LANES), 0)
    evens, odds = [], []
    for block in range(half // SEGMENTS):
        near = 2 * SEGMENTS * block
        direct = table_ref[pl.ds(near, SEGMENTS, stride=2), :]
        if block == 0:
            mirror = turned(table_ref[pl.ds(full - 2 * SEGMENTS, SEGMENTS, stride=2), :])
            mirror = jnp.where(row == 0, 0.0, pltpu.roll(mirror, 1, 0))
        else:
            mirror = turned(table_ref[pl.ds(full - near - 14, SEGMENTS, stride=2), :])
        evens.append(direct + mirror)
        direct = table_ref[pl.ds(near + 1, SEGMENTS, stride=2), :]
        mirror = turned(table_ref[pl.ds(full - near - 15, SEGMENTS, stride=2), :])
        odds.append(-(direct + mirror))
    return (
        jnp.concatenate(evens, axis=0),
        jnp.concatenate(odds, axis=0),
        table_ref[pl.ds(2 * half, 1), :],
    )


def wide(column, columns):
    return jnp.concatenate([column] * (columns // LANES), axis=1)


def one_minus_exp(x):
    series = jnp.ones_like(x)
    for term in range(9, 1, -1):
        series = 1.0 - x * series * (1.0 / term)
    return jnp.where(x < 0.4, x * series, 1.0 - jnp.exp(-x))


def spread(burst_ref, rows_ref, blocks_ref, out_ref):
    placed = jnp.dot(
        rows_ref[...] * burst_ref[...].reshape(1, -1), blocks_ref[...],
        precision=lax.Precision.HIGHEST, preferred_element_type=jnp.float32,
    )
    for block in range(placed.shape[1]):
        out_ref[pl.ds(block * SEGMENTS, SEGMENTS), :] = jnp.broadcast_to(
            placed[:, block : block + 1], (SEGMENTS, LANES)
        )


def orders(blocks):
    return (
        (range(blocks // 2), range(SEGMENTS)),
        (range(blocks - 1, blocks // 2 - 1, -1), range(SEGMENTS - 1, -1, -1)),
    )


def rows_of(block):
    return pl.ds(block * SEGMENTS, SEGMENTS)


def columns_of(step):
    return pl.ds(pl.multiple_of(step * BLOCK, BLOCK), BLOCK)


def scan(series, factors_ref, keep, fresh, states_ref=None):
    columns = keep.shape[1]
    entering = jnp.zeros((1, columns), jnp.float32)
    for order, rows in orders(factors_ref.shape[0] // SEGMENTS):
        state = decay = None
        for block in order:
            burst = factors_ref[rows_of(block), :]
            power = burst * burst
            variance = wide(1.0 - power, columns) + wide(power, columns) * fresh
            kick = variance * lax.rsqrt(variance) * series(block)
            factor = wide(burst, columns) * keep
            state = kick if state is None else factor * state + kick
            decay = factor if decay is None else factor * decay
            if states_ref is not None:
                states_ref[rows_of(block), :] = state
        before = [None] * SEGMENTS
        for row in rows:
            before[row] = entering
            entering = decay[row : row + 1] * entering + state[row : row + 1]
        if states_ref is not None:
            value = jnp.concatenate(before, axis=0)
            for block in order:
                value = wide(factors_ref[rows_of(block), :], columns) * keep * value
                states_ref[rows_of(block), :] += value
    return entering


def own_kernel(section_ref, *refs):
    count = BLOCK // LANES
    quarter_refs = refs[:count]
    rate_ref, burst_ref, rows_ref, blocks_ref = refs[count : count + 4]
    sources = refs[count + 4 : count + 11]
    (
        series_ref, after_ref, scale_ref, ends_ref, factors_ref, gains_ref,
        rows_kept_ref, blocks_kept_ref, *kept,
    ) = refs[count + 11 : count + 22]
    *own_tables, semaphores = refs[count + 22 :]
    even_cos_ref, even_sin_ref, odd_cos_ref, odd_sin_ref = own_tables
    forward_ref, sums_ref, differences_ref = kept
    targets = (forward_ref, *own_tables, sums_ref, differences_ref)
    copies = [
        pltpu.make_async_copy(source, target, semaphores.at[place])
        for place, (source, target) in enumerate(zip(sources, targets))
    ]
    step = pl.program_id(0)

    @pl.when(step == 0)
    def _():
        for copy in copies:
            copy.start()
        spread(burst_ref, rows_ref, blocks_ref, factors_ref)
        rows_kept_ref[...] = rows_ref[...]
        blocks_kept_ref[...] = blocks_ref[...]
        for copy in copies[:-2]:
            copy.wait()

    @pl.when(step == pl.num_programs(0) - 1)
    def _():
        for copy in copies[-2:]:
            copy.wait()

    series_ref, after_ref, scale_ref = (x.at[step] for x in (series_ref, after_ref, scale_ref))
    length, columns = section_ref.shape
    half = length // 2
    segment = half // SEGMENTS
    evens, odds, nyquist = (
        jnp.concatenate(part, axis=1) for part in zip(*map(mirrored, quarter_refs))
    )
    scale_ref[pl.ds(0, half), :] = evens
    scale_ref[pl.ds(half, half), :] = odds
    scale_ref[pl.ds(length, SEGMENTS), :] = jnp.broadcast_to(nyquist, (SEGMENTS, columns))
    even_cos, even_sin, odd_cos, odd_sin = (
        dot(table_ref[...], part)
        for table_ref, part in zip(
            own_tables, spectra(section_ref[...], evens, nyquist, odds, forward_ref)
        )
    )
    for block in range(segment + 1):
        at = slice(block * SEGMENTS, (block + 1) * SEGMENTS)
        ec, es, oc, os = even_cos[at], even_sin[at], odd_cos[at], odd_sin[at]
        if block < segment:
            even, odd = ec + es, oc + os
            series_ref[rows_of(block), :] = even - odd
            after_ref[rows_of(block), :] = even + odd
        if block > 0:
            even, odd = ec - es, os - oc
            series_ref[rows_of(segment + block - 1), :] = even - odd
            after_ref[rows_of(segment + block - 1), :] = even + odd
    rate = rate_ref[...]
    keep = jnp.exp(-rate)
    fresh = one_minus_exp(2.0 * rate)
    at = columns_of(step)
    gains_ref[pl.ds(0, 1), at] = keep
    gains_ref[pl.ds(1, 1), at] = fresh
    ends_ref[pl.ds(0, 1), at] = scan(
        lambda block: series_ref[rows_of(block), :], factors_ref, keep, fresh
    )
    logs = jnp.sum(jnp.log(factors_ref[...]), axis=0, keepdims=True)
    ends_ref[pl.ds(1, 1), at] = jnp.exp(wide(logs, columns) - length * rate)


def next_kernel(after_ref, ends_ref, gains_ref, burst_ref, rows_ref, blocks_ref, out_ref, factors_ref):
    step = pl.program_id(0)

    @pl.when(step == 0)
    def _():
        spread(burst_ref, rows_ref, blocks_ref, factors_ref)

    after_ref = after_ref.at[step]
    columns = after_ref.shape[1]
    at = columns_of(step)
    out_ref[pl.ds(0, 1), at] = ends_ref[pl.ds(0, 1), at]
    out_ref[pl.ds(1, 1), at] = scan(
        lambda block: after_ref[rows_of(block), :], factors_ref,
        gains_ref[pl.ds(0, 1), at], gains_ref[pl.ds(1, 1), at],
    )
    out_ref[pl.ds(2, 1), at] = ends_ref[pl.ds(1, 1), at]
    out_ref[pl.ds(3, 1), at] = jnp.ones((1, columns), jnp.float32)


def merge_kernel(step, sent_ref, got_ref, *refs):
    *before_ref, out_ref, after_ref = refs
    later = (lax.axis_index("tm") // step) % 2 == 1
    sent, got = sent_ref[...], got_ref[...]
    low = jnp.where(later, got, sent)
    high = jnp.where(later, sent, got)
    out_ref[pl.ds(0, 1), :] = high[:1] + high[2:3] * low[:1] + high[3:] * low[1:2]
    out_ref[pl.ds(1, 1), :] = high[1:2]
    out_ref[pl.ds(2, 1), :] = high[2:3] * low[2:3]
    out_ref[pl.ds(3, 1), :] = high[2:3] * low[3:]
    if before_ref:
        before, decay, decay_later = (before_ref[0][pl.ds(row, 1), :] for row in range(3))
    else:
        decay = jnp.ones_like(sent[:1])
        before = decay_later = jnp.zeros_like(decay)
    added = before + decay * got[:1] + decay_later * got[1:2]
    after_ref[pl.ds(0, 1), :] = jnp.where(later, added, before)
    after_ref[pl.ds(1, 1), :] = jnp.where(later, decay * got[2:3], decay)
    after_ref[pl.ds(2, 1), :] = jnp.where(later, decay * got[3:], decay_later)


def middle_kernel(
    first, section_ref, gains_ref, scale_ref, series_ref, factors_ref, forward_ref, sums_ref,
    differences_ref, *refs,
):
    *_, states_ref, work_ref = refs
    step = first + pl.program_id(0)
    at_columns = columns_of(step)
    scale_ref, series_ref, states_ref = (x.at[step] for x in (scale_ref, series_ref, states_ref))
    length = section_ref.shape[0]
    half = length // 2
    segment = half // SEGMENTS
    even_cos, even_sin, odd_cos, odd_sin = spectra(
        section_ref[:, at_columns],
        scale_ref[pl.ds(0, half), :],
        scale_ref[pl.ds(length, 1), :],
        scale_ref[pl.ds(half, half), :],
        forward_ref,
    )
    sums = dot(sums_ref[...], jnp.concatenate([even_cos, odd_sin], axis=0))
    differences = dot(differences_ref[...], jnp.concatenate([even_sin, odd_cos], axis=0))
    for block in range(segment + 1):
        at = slice(block * SEGMENTS, (block + 1) * SEGMENTS)
        if block < segment:
            place = rows_of(block)
            work_ref[place, :] = sums[at] + differences[at] + series_ref[place, :]
        if block > 0:
            place = rows_of(segment + block - 1)
            work_ref[place, :] = sums[at] - differences[at] + series_ref[place, :]
    scan(
        lambda block: work_ref[rows_of(block), :], factors_ref,
        gains_ref[pl.ds(0, 1), at_columns], gains_ref[pl.ds(1, 1), at_columns], states_ref,
    )


def last_kernel(states_ref, gains_ref, factors_ref, sent_ref, before_ref, out_ref, order_ref):
    step = pl.program_id(0)
    at = columns_of(step)
    states_ref = states_ref.at[step]
    length, columns = states_ref.shape
    blocks = length // SEGMENTS
    segment = blocks // 2
    keep = gains_ref[pl.ds(0, 1), at]
    state, spill, total, later = (sent_ref[pl.ds(row, 1), at] for row in range(4))
    before, decay, decay_later = (before_ref[pl.ds(row, 1), at] for row in range(3))
    opening = (state + later * spill) / (1.0 - total)
    entering = before + decay * opening + decay_later * spill
    for order, rows in orders(blocks):
        decay = None
        for block in order:
            factor = wide(factors_ref[rows_of(block), :], columns) * keep
            decay = factor if decay is None else factor * decay
        values = [None] * SEGMENTS
        for row in rows:
            values[row] = entering
            entering = decay[row : row + 1] * entering
        value = jnp.concatenate(values, axis=0)
        for block in order:
            value = wide(factors_ref[rows_of(block), :], columns) * keep * value
            result = states_ref[rows_of(block), :] + value
            if block < segment:
                first = block
            else:
                result = turned(result)
                first = length - 1 - (block - segment) - (SEGMENTS - 1) * segment
            for lane in range(columns // LANES):
                order_ref[lane, pl.ds(first, SEGMENTS, stride=segment), :] = result[
                    :, lane * LANES : (lane + 1) * LANES
                ]
    for lane in range(columns // LANES):
        out_ref[:, lane * LANES : (lane + 1) * LANES] = order_ref[lane]


VMEM = pl.BlockSpec(memory_space=pltpu.VMEM)
HBM = pl.BlockSpec(memory_space=pltpu.HBM)


def whole(array):
    return pl.BlockSpec(array.shape, lambda i: (0,) * array.ndim)


def blocks(rows):
    return pl.BlockSpec((rows, BLOCK), lambda i: (0, i))


def quarters(rows):
    count = BLOCK // LANES
    return [
        pl.BlockSpec((rows, LANES), lambda i, place=place: (0, count * i + place))
        for place in range(count)
    ]


def in_hbm(array):
    return pltpu.with_memory_space_constraint(array, pltpu.HBM)


def cost(flops):
    return pl.CostEstimate(flops=flops, bytes_accessed=2**24, transcendentals=0)


def params(mebibytes):
    return pltpu.CompilerParams(vmem_limit_bytes=mebibytes * 2**20)


def shards(constants, random_forcing, eigen_root_table, lane_fading_speed, sudden_shrink):
    tables, (rows, places) = constants[:7], constants[7:]
    length, channels = random_forcing.shape
    count = lax.axis_size("tm")
    steps = channels // BLOCK
    ahead = [(i, (i + 1) % count) for i in range(count)]
    back = [((i + 1) % count, i) for i in range(count)]
    rate = lane_fading_speed[None, :]
    work = 2 * channels * length * length

    previous = lax.ppermute(random_forcing, "tm", ahead)
    following = lax.ppermute(sudden_shrink, "tm", back)

    def vmem(*shape, dtype=jnp.float32):
        return pltpu.VMEM(shape, dtype)

    def kept(table):
        return vmem(*table.shape, dtype=table.dtype)

    (
        series, after, scale, ends, factors, gains, rows, places, *middle_tables
    ) = pl.pallas_call(
        own_kernel,
        grid=(steps,),
        in_specs=[
            blocks(length), *quarters(2 * length), blocks(1), whole(sudden_shrink),
            whole(rows), whole(places), *[HBM] * 7,
        ],
        out_specs=[VMEM] * 11,
        out_shape=[
            vmem(steps, length, BLOCK), vmem(steps, length, BLOCK),
            vmem(steps, length + SEGMENTS, BLOCK), vmem(SEGMENTS, channels),
            vmem(length, LANES), vmem(SEGMENTS, channels),
            *map(kept, (rows, places, tables[0], *tables[5:])),
        ],
        scratch_shapes=[
            *(kept(table) for table in tables[1:5]), pltpu.SemaphoreType.DMA((7,)),
        ],
        compiler_params=params(36),
        cost_estimate=cost(7 * work),
        name="own",
    )(
        *map(
            in_hbm,
            (
                random_forcing, *[eigen_root_table] * (BLOCK // LANES), rate, sudden_shrink,
                rows, places, *tables,
            ),
        )
    )

    sent = pl.pallas_call(
        next_kernel,
        grid=(steps,),
        in_specs=[VMEM] * 6,
        out_specs=VMEM,
        out_shape=vmem(4, channels),
        scratch_shapes=[vmem(length, LANES)],
        compiler_params=params(16),
        cost_estimate=cost(work),
        name="next",
    )(after, ends, gains, following, rows, places)

    states = ()
    for part in range(2):
        states = (
            pl.pallas_call(
                functools.partial(middle_kernel, part * steps // 2),
                grid=(steps // 2,),
                in_specs=[VMEM] * (8 + len(states)),
                out_specs=VMEM,
                out_shape=vmem(steps, length, BLOCK),
                scratch_shapes=[vmem(length, BLOCK)],
                input_output_aliases={8: 0} if states else {},
                compiler_params=params(24),
                cost_estimate=cost(4 * work),
                name="middle",
            )(previous, gains, scale, series, factors, *middle_tables, *states),
        )
    (states,) = states

    before = None
    step = 1
    while step < count:
        got = lax.ppermute(sent, "tm", [(i, i ^ step) for i in range(count)])
        kept_rows = () if before is None else (before,)
        sent, before = pl.pallas_call(
            functools.partial(merge_kernel, step),
            in_specs=[VMEM] * (2 + len(kept_rows)),
            out_specs=[VMEM] * 2,
            out_shape=[vmem(4, channels), vmem(3, channels)],
            compiler_params=params(4),
            cost_estimate=cost(channels),
            name="merge",
        )(sent, got, *kept_rows)
        step *= 2

    return pl.pallas_call(
        last_kernel,
        grid=(steps,),
        in_specs=[VMEM] * 5,
        out_specs=blocks(length),
        out_shape=pltpu.HBM((length, channels), jnp.float32),
        scratch_shapes=[vmem(BLOCK // LANES, length, LANES)],
        compiler_params=params(16),
        cost_estimate=cost(work),
        name="last",
    )(states, gains, factors, sent, before)


def solution(mesh):
    placed = (P("tm", "chan"), P(None, "chan"), P("chan"), P("tm"))

    def program(random_forcing, eigen_root_table, lane_fading_speed, sudden_shrink):
        length = random_forcing.shape[0] // mesh.shape["tm"]
        constants = tuple(jnp.asarray(table) for table in tables(length))

        def body(*args):
            return shards(args[:-4], *args[-4:])

        return jax.shard_map(
            body, mesh=mesh, in_specs=(P(None, None),) * len(constants) + placed,
            out_specs=P("tm", "chan"), check_vma=False,
        )(*constants, random_forcing, eigen_root_table, lane_fading_speed, sudden_shrink)

    return program
```

```python
import functools

import jax
import jax.numpy as jnp
import numpy as np
from jax import lax
from jax.experimental import pallas as pl
from jax.experimental.pallas import tpu as pltpu
from jax.sharding import PartitionSpec as P

LANES = 128
SEGMENTS = 8
BLOCK = 512
NYQUIST_ROWS = 16


def split(table):
    high = table.astype(jnp.bfloat16)
    low = (table - high.astype(np.float64)).astype(jnp.bfloat16)
    return high, low


def tripled(table):
    high, low = split(table)
    return np.concatenate([high, high, low], axis=1)


def tables(length):
    full = 2 * length
    half = length // 2
    frequency = 2 * np.arange(half)[:, None]
    nyquist = np.full((1, 1), length)

    def angle(frequencies, times):
        return (frequencies * times[None, :] % full) * (2.0 * np.pi / full)

    def parts(times):
        blank = np.zeros((NYQUIST_ROWS - 1, times.size))
        return (
            np.concatenate([np.cos(angle(frequency, times)), np.cos(angle(nyquist, times)), blank]),
            np.sin(angle(frequency, times)),
            np.cos(angle(frequency + 1, times)),
            np.sin(angle(frequency + 1, times)),
        )

    forward = np.concatenate(split(np.concatenate(parts(np.arange(length)))), axis=1)
    ticks = np.arange(length)
    counted = np.where(ticks < half, ticks, length - 1 - ticks)
    segment = half // SEGMENTS
    times = (np.arange(segment + 1)[:, None] + segment * np.arange(SEGMENTS)[None, :]).reshape(-1)
    even_cos, even_sin, odd_cos, odd_sin = (tripled(part.T / full) for part in parts(times))
    rows = counted // segment == np.arange(SEGMENTS)[:, None]
    blocks = counted % segment + np.where(ticks < half, 0, segment)
    blocks = blocks[:, None] == np.arange(2 * segment)
    return (
        forward, even_cos, even_sin, odd_cos, odd_sin,
        rows.astype(np.float32), blocks.astype(np.float32),
    )


def dot(left, right):
    return jnp.dot(left, right, preferred_element_type=jnp.float32)


def stacked(values):
    high = values.astype(jnp.bfloat16)
    low = (values - high.astype(jnp.float32)).astype(jnp.bfloat16)
    return jnp.concatenate([high, low, high], axis=0)


def spectra(section, evens, nyquist, odds, forward_ref):
    half = section.shape[0] // 2
    doubled = jnp.concatenate([section, section], axis=0)
    first = half + NYQUIST_ROWS
    scale = jnp.concatenate(
        [evens, jnp.broadcast_to(nyquist, (NYQUIST_ROWS, evens.shape[1]))], axis=0
    )
    even_cos = stacked(dot(forward_ref[:first], doubled) * scale)
    starts = (first, first + half, first + 2 * half)
    even_sin, odd_cos, odd_sin = (
        stacked(dot(forward_ref[at : at + half], doubled) * scale)
        for at, scale in zip(starts, (evens, odds, odds))
    )
    return even_cos, even_sin, odd_cos, odd_sin


def turned(x):
    row = lax.broadcasted_iota(jnp.int32, x.shape, 0)
    return jnp.take_along_axis(x, SEGMENTS - 1 - row, axis=0, mode="promise_in_bounds")


def mirrored(table_ref):
    full = table_ref.shape[0]
    half = full // 4
    row = lax.broadcasted_iota(jnp.int32, (SEGMENTS, LANES), 0)
    evens, odds = [], []
    for block in range(half // SEGMENTS):
        near = 2 * SEGMENTS * block
        direct = table_ref[pl.ds(near, SEGMENTS, stride=2), :]
        if block == 0:
            mirror = turned(table_ref[pl.ds(full - 2 * SEGMENTS, SEGMENTS, stride=2), :])
            mirror = jnp.where(row == 0, 0.0, pltpu.roll(mirror, 1, 0))
        else:
            mirror = turned(table_ref[pl.ds(full - near - 14, SEGMENTS, stride=2), :])
        evens.append(direct + mirror)
        direct = table_ref[pl.ds(near + 1, SEGMENTS, stride=2), :]
        mirror = turned(table_ref[pl.ds(full - near - 15, SEGMENTS, stride=2), :])
        odds.append(-(direct + mirror))
    return (
        jnp.concatenate(evens, axis=0),
        jnp.concatenate(odds, axis=0),
        table_ref[pl.ds(2 * half, 1), :],
    )


def wide(column, columns):
    return jnp.concatenate([column] * (columns // LANES), axis=1)


def one_minus_exp(x):
    series = jnp.ones_like(x)
    for term in range(9, 1, -1):
        series = 1.0 - x * series * (1.0 / term)
    return jnp.where(x < 0.4, x * series, 1.0 - jnp.exp(-x))


def spread(burst_ref, rows_ref, blocks_ref, out_ref):
    placed = jnp.dot(
        rows_ref[...] * burst_ref[...].reshape(1, -1), blocks_ref[...],
        precision=lax.Precision.HIGHEST, preferred_element_type=jnp.float32,
    )
    for block in range(placed.shape[1]):
        out_ref[pl.ds(block * SEGMENTS, SEGMENTS), :] = jnp.broadcast_to(
            placed[:, block : block + 1], (SEGMENTS, LANES)
        )


def orders(blocks):
    return (
        (range(blocks // 2), range(SEGMENTS)),
        (range(blocks - 1, blocks // 2 - 1, -1), range(SEGMENTS - 1, -1, -1)),
    )


def rows_of(block):
    return pl.ds(block * SEGMENTS, SEGMENTS)


def columns_of(step):
    return pl.ds(pl.multiple_of(step * BLOCK, BLOCK), BLOCK)


def scan(series, factors_ref, keep, fresh, states_ref=None, store=None):
    columns = keep.shape[1]
    entering = jnp.zeros((1, columns), jnp.float32)
    for order, rows in orders(factors_ref.shape[0] // SEGMENTS):
        state = decay = None
        for block in order:
            burst = factors_ref[rows_of(block), :]
            power = burst * burst
            variance = wide(1.0 - power, columns) + wide(power, columns) * fresh
            kick = variance * lax.rsqrt(variance) * series(block)
            factor = wide(burst, columns) * keep
            state = kick if state is None else factor * state + kick
            decay = factor if decay is None else factor * decay
            if states_ref is not None:
                states_ref[rows_of(block), :] = state
        before = [None] * SEGMENTS
        for row in rows:
            before[row] = entering
            entering = decay[row : row + 1] * entering + state[row : row + 1]
        if states_ref is not None:
            value = jnp.concatenate(before, axis=0)
            for block in order:
                value = wide(factors_ref[rows_of(block), :], columns) * keep * value
                store(block, states_ref[rows_of(block), :] + value)
    return entering


def load_kernel(section_hbm, table_hbm, rate_hbm, burst_hbm, *refs):
    sources, refs = refs[:7], refs[7:]
    part_refs, refs = refs[:3], refs[3:]
    table_ref, factors_ref, powers_ref, gains_ref = refs[:4]
    targets, (rate_ref, burst_ref, semaphores) = refs[4:11], refs[11:]
    length, channels = section_hbm.shape
    starts = (0, part_refs[0].shape[1], channels - part_refs[2].shape[1])
    copies = [
        pltpu.make_async_copy(source, target, semaphores.at[place])
        for place, (source, target) in enumerate(
            [(burst_hbm, burst_ref), *zip(sources[:2], targets[:2]), (rate_hbm, rate_ref)]
            + [
                (section_hbm.at[:, pl.ds(start, part_ref.shape[1])], part_ref)
                for start, part_ref in zip(starts, part_refs)
            ]
            + [
                (table_hbm.at[:, pl.ds(group * LANES, LANES)], table_ref.at[group])
                for group in range(BLOCK // LANES)
            ]
            + list(zip(sources[2:], targets[2:]))
        )
    ]
    for copy in copies:
        copy.start()
    for copy in copies[:4]:
        copy.wait()
    rows_ref, blocks_ref = targets[:2]
    spread(burst_ref, rows_ref, blocks_ref, factors_ref)
    shape = (length, length)
    earlier = lax.broadcasted_iota(jnp.int32, shape, 1) <= lax.broadcasted_iota(jnp.int32, shape, 0)
    logs = jnp.where(earlier, jnp.log(burst_ref[...].reshape(1, -1)), 0.0)
    powers_ref[...] = jnp.broadcast_to(
        jnp.exp(jnp.sum(logs, axis=1, keepdims=True)), (length, LANES)
    )
    rate = rate_ref[...]
    keep = jnp.exp(-rate)
    gains_ref[pl.ds(0, 1), :] = keep
    gains_ref[pl.ds(1, 1), :] = one_minus_exp(2.0 * rate)
    total = jnp.sum(jnp.log(factors_ref[...]), axis=0, keepdims=True)
    gains_ref[pl.ds(2, 1), :] = jnp.exp(wide(total, rate.shape[1]) - length * rate)
    for copy in copies[4:]:
        copy.wait()


def own_kernel(section_hbm, table_hbm, part_ref, first_ref, factors_ref, gains_ref, forward_ref, *refs):
    own_tables, refs = refs[:4], refs[4:]
    series_ref, after_ref, scale_ref, ends_ref, sums_ref, differences_ref = refs[:6]
    section_ref, table_ref, section_semaphores, table_semaphores = refs[6:]
    even_cos_ref, even_sin_ref, odd_cos_ref, odd_sin_ref = own_tables
    step = pl.program_id(0)
    length, channels = section_ref.shape
    half = length // 2
    segment = half // SEGMENTS
    groups = BLOCK // LANES

    def load_section(block):
        return pltpu.make_async_copy(
            section_hbm.at[:, columns_of(block)], section_ref.at[:, columns_of(block)],
            section_semaphores.at[block],
        )

    def load_table(group):
        columns = pl.ds(pl.multiple_of(group * LANES, LANES), LANES)
        return pltpu.make_async_copy(
            table_hbm.at[:, columns], table_ref.at[group], table_semaphores.at[group]
        )

    @pl.when(step == 0)
    def _():
        for block in range(1, channels // BLOCK):
            load_section(block).start()
            for group in range(groups):
                load_table(block * groups + group).start()
        section_ref[:, :BLOCK] = part_ref[:, :BLOCK]
        for group in range(groups):
            table_ref[group] = first_ref[group]

    @pl.when(step == pl.num_programs(0) - 1)
    def _():
        for target, first, second in (
            (sums_ref, even_cos_ref, odd_sin_ref), (differences_ref, even_sin_ref, odd_cos_ref)
        ):
            target[:, : first.shape[1]] = first[...]
            target[:, first.shape[1] :] = second[...]

    @pl.when(step > 0)
    def _():
        load_section(step).wait()
        for group in range(groups):
            load_table(step * groups + group).wait()

    for block in (step,):
        series, after, scale = (x.at[block] for x in (series_ref, after_ref, scale_ref))
        at = columns_of(block)
        evens, odds, nyquist = (
            jnp.concatenate(part, axis=1)
            for part in zip(
                *(mirrored(table_ref.at[block * groups + group]) for group in range(groups))
            )
        )
        scale[pl.ds(0, half), :] = evens
        scale[pl.ds(half, half), :] = odds
        scale[pl.ds(length, SEGMENTS), :] = jnp.broadcast_to(nyquist, (SEGMENTS, BLOCK))
        even_cos, even_sin, odd_cos, odd_sin = (
            dot(inverse_ref[...], part)
            for inverse_ref, part in zip(
                own_tables, spectra(section_ref[:, at], evens, nyquist, odds, forward_ref)
            )
        )
        for row in range(segment + 1):
            rows = slice(row * SEGMENTS, (row + 1) * SEGMENTS)
            ec, es, oc, os = even_cos[rows], even_sin[rows], odd_cos[rows], odd_sin[rows]
            if row < segment:
                even, odd = ec + es, oc + os
                series[rows_of(row), :] = even - odd
                after[rows_of(row), :] = even + odd
            if row > 0:
                even, odd = ec - es, os - oc
                series[rows_of(segment + row - 1), :] = even - odd
                after[rows_of(segment + row - 1), :] = even + odd
        ends_ref[pl.ds(0, 1), at] = scan(
            lambda row: series[rows_of(row), :], factors_ref,
            gains_ref[pl.ds(0, 1), at], gains_ref[pl.ds(1, 1), at],
        )


def next_kernel(after_ref, ends_ref, gains_ref, burst_ref, rows_ref, blocks_ref, out_ref, factors_ref):
    step = pl.program_id(0)

    @pl.when(step == 0)
    def _():
        spread(burst_ref, rows_ref, blocks_ref, factors_ref)

    after_ref = after_ref.at[step]
    columns = after_ref.shape[1]
    at = columns_of(step)
    out_ref[pl.ds(0, 1), at] = ends_ref[pl.ds(0, 1), at]
    out_ref[pl.ds(1, 1), at] = scan(
        lambda block: after_ref[rows_of(block), :], factors_ref,
        gains_ref[pl.ds(0, 1), at], gains_ref[pl.ds(1, 1), at],
    )
    out_ref[pl.ds(2, 1), at] = gains_ref[pl.ds(2, 1), at]
    out_ref[pl.ds(3, 1), at] = jnp.ones((1, columns), jnp.float32)


def merge_kernel(step, sent_ref, got_ref, *refs):
    *before_ref, out_ref, after_ref = refs
    later = (lax.axis_index("tm") // step) % 2 == 1
    sent, got = sent_ref[...], got_ref[...]
    low = jnp.where(later, got, sent)
    high = jnp.where(later, sent, got)
    out_ref[pl.ds(0, 1), :] = high[:1] + high[2:3] * low[:1] + high[3:] * low[1:2]
    out_ref[pl.ds(1, 1), :] = high[1:2]
    out_ref[pl.ds(2, 1), :] = high[2:3] * low[2:3]
    out_ref[pl.ds(3, 1), :] = high[2:3] * low[3:]
    if before_ref:
        before, decay, decay_later = (before_ref[0][pl.ds(row, 1), :] for row in range(3))
    else:
        decay = jnp.ones_like(sent[:1])
        before = decay_later = jnp.zeros_like(decay)
    added = before + decay * got[:1] + decay_later * got[1:2]
    after_ref[pl.ds(0, 1), :] = jnp.where(later, added, before)
    after_ref[pl.ds(1, 1), :] = jnp.where(later, decay * got[2:3], decay)
    after_ref[pl.ds(2, 1), :] = jnp.where(later, decay * got[3:], decay_later)


def middle_kernel(
    first, section_ref, gains_ref, scale_ref, series_ref, factors_ref, forward_ref, sums_ref,
    differences_ref, *refs,
):
    *_, states_ref, work_ref = refs
    step = first + pl.program_id(0)
    at_columns = columns_of(step)
    scale_ref, series_ref = scale_ref.at[step], series_ref.at[step]
    length = section_ref.shape[0]
    half = length // 2
    segment = half // SEGMENTS
    even_cos, even_sin, odd_cos, odd_sin = spectra(
        section_ref[:, columns_of(step - first)],
        scale_ref[pl.ds(0, half), :],
        scale_ref[pl.ds(length, 1), :],
        scale_ref[pl.ds(half, half), :],
        forward_ref,
    )
    sums = dot(sums_ref[...], jnp.concatenate([even_cos, odd_sin], axis=0))
    differences = dot(differences_ref[...], jnp.concatenate([even_sin, odd_cos], axis=0))
    for block in range(segment + 1):
        at = slice(block * SEGMENTS, (block + 1) * SEGMENTS)
        if block < segment:
            place = rows_of(block)
            work_ref[place, :] = sums[at] + differences[at] + series_ref[place, :]
        if block > 0:
            place = rows_of(segment + block - 1)
            work_ref[place, :] = sums[at] - differences[at] + series_ref[place, :]
    groups = BLOCK // LANES

    def store(block, value):
        if block < segment:
            start = block
        else:
            value = turned(value)
            start = length - 1 - (block - segment) - (SEGMENTS - 1) * segment
        for group in range(groups):
            states_ref[step * groups + group, pl.ds(start, SEGMENTS, stride=segment), :] = value[
                :, group * LANES : (group + 1) * LANES
            ]

    scan(
        lambda block: work_ref[rows_of(block), :], factors_ref,
        gains_ref[pl.ds(0, 1), at_columns], gains_ref[pl.ds(1, 1), at_columns], work_ref, store,
    )


def last_kernel(states_ref, gains_ref, powers_ref, sent_ref, before_ref, out_ref):
    step = pl.program_id(0)
    at = columns_of(step)
    length, columns = out_ref.shape
    keep = gains_ref[pl.ds(0, 1), at]
    state, spill, total, later = (sent_ref[pl.ds(row, 1), at] for row in range(4))
    before, decay, decay_later = (before_ref[pl.ds(row, 1), at] for row in range(3))
    opening = (state + later * spill) / (1.0 - total)
    entering = before + decay * opening + decay_later * spill
    rows = []
    for _ in range(SEGMENTS):
        entering = keep * entering
        rows.append(entering)
    value = jnp.concatenate(rows, axis=0)
    jump = keep
    for _ in range(SEGMENTS.bit_length() - 1):
        jump = jump * jump
    groups = columns // LANES
    for block in range(length // SEGMENTS):
        place = rows_of(block)
        states = jnp.concatenate(
            [states_ref[step * groups + group, place, :] for group in range(groups)], axis=1
        )
        out_ref[place, :] = states + wide(powers_ref[place, :], columns) * value
        value = jump * value


VMEM = pl.BlockSpec(memory_space=pltpu.VMEM)
HBM = pl.BlockSpec(memory_space=pltpu.HBM)


def in_hbm(array):
    return pltpu.with_memory_space_constraint(array, pltpu.HBM)


def cost(flops):
    return pl.CostEstimate(flops=flops, bytes_accessed=2**24, transcendentals=0)


def params(mebibytes):
    return pltpu.CompilerParams(vmem_limit_bytes=mebibytes * 2**20)


def shards(constants, random_forcing, eigen_root_table, lane_fading_speed, sudden_shrink):
    tables, (rows, places) = constants[:5], constants[5:]
    length, channels = random_forcing.shape
    count = lax.axis_size("tm")
    steps = channels // BLOCK
    ahead = [(i, (i + 1) % count) for i in range(count)]
    back = [((i + 1) % count, i) for i in range(count)]
    rate = lane_fading_speed[None, :]
    work = 2 * channels * length * length

    def vmem(*shape, dtype=jnp.float32):
        return pltpu.VMEM(shape, dtype)

    def kept(table):
        return vmem(*table.shape, dtype=table.dtype)

    def joined(pair):
        return vmem(
            pair[0].shape[0], sum(table.shape[1] for table in pair), dtype=pair[0].dtype
        )

    cuts = (0, steps // 2, steps - max(1, steps // 4), steps)
    loaded = pl.pallas_call(
        load_kernel,
        in_specs=[HBM] * 11,
        out_specs=[VMEM] * 14,
        out_shape=[
            *(
                vmem(length, width * BLOCK, dtype=random_forcing.dtype)
                for width in (end - start for start, end in zip(cuts, cuts[1:]))
            ),
            vmem(BLOCK // LANES, 2 * length, LANES), vmem(length, LANES), vmem(length, LANES),
            vmem(SEGMENTS, channels), *map(kept, (rows, places, *tables)),
        ],
        scratch_shapes=[vmem(1, channels), vmem(length), pltpu.SemaphoreType.DMA((16,))],
        compiler_params=params(8),
        cost_estimate=cost(work // 4),
        name="load",
    )(*map(in_hbm, (random_forcing, eigen_root_table, rate, sudden_shrink, rows, places, *tables)))

    parts, inverses = loaded[:3], loaded[10:]
    first, factors, powers, gains, rows, places, forward = loaded[3:10]
    previous = []
    for part in range(3):
        previous.append(lax.ppermute(parts[part], "tm", ahead))
    following = lax.ppermute(sudden_shrink, "tm", back)

    series, after, scale, ends, *middle_tables = pl.pallas_call(
        own_kernel,
        grid=(steps,),
        in_specs=[HBM] * 2 + [VMEM] * 9,
        out_specs=[VMEM] * 6,
        out_shape=[
            vmem(steps, length, BLOCK), vmem(steps, length, BLOCK),
            vmem(steps, length + SEGMENTS, BLOCK), vmem(1, channels),
            *map(joined, (inverses[::3], inverses[1:3])),
        ],
        scratch_shapes=[
            kept(random_forcing), vmem(channels // LANES, 2 * length, LANES),
            pltpu.SemaphoreType.DMA((steps,)), pltpu.SemaphoreType.DMA((channels // LANES,)),
        ],
        compiler_params=params(22),
        cost_estimate=cost(7 * work),
        name="own",
    )(
        in_hbm(random_forcing), in_hbm(eigen_root_table), parts[0], first, factors, gains,
        forward, *inverses,
    )

    sent = pl.pallas_call(
        next_kernel,
        grid=(steps,),
        in_specs=[VMEM] * 6,
        out_specs=VMEM,
        out_shape=vmem(4, channels),
        scratch_shapes=[vmem(length, LANES)],
        compiler_params=params(16),
        cost_estimate=cost(work),
        name="next",
    )(after, ends, gains, following, rows, places)

    states = ()
    for part, (first, end) in enumerate(zip(cuts, cuts[1:])):
        states = (
            pl.pallas_call(
                functools.partial(middle_kernel, first),
                grid=(end - first,),
                in_specs=[VMEM] * (8 + len(states)),
                out_specs=VMEM,
                out_shape=vmem(channels // LANES, length, LANES),
                scratch_shapes=[vmem(length, BLOCK)],
                input_output_aliases={8: 0} if states else {},
                compiler_params=params(24),
                cost_estimate=cost(4 * work),
                name="middle",
            )(previous[part], gains, scale, series, factors, forward, *middle_tables, *states),
        )
    (states,) = states

    before = None
    step = 1
    while step < count:
        got = lax.ppermute(sent, "tm", [(i, i ^ step) for i in range(count)])
        kept_rows = () if before is None else (before,)
        sent, before = pl.pallas_call(
            functools.partial(merge_kernel, step),
            in_specs=[VMEM] * (2 + len(kept_rows)),
            out_specs=[VMEM] * 2,
            out_shape=[vmem(4, channels), vmem(3, channels)],
            compiler_params=params(4),
            cost_estimate=cost(channels),
            name="merge",
        )(sent, got, *kept_rows)
        step *= 2

    return pl.pallas_call(
        last_kernel,
        grid=(steps,),
        in_specs=[VMEM] * 5,
        out_specs=pl.BlockSpec((length, BLOCK), lambda i: (0, i)),
        out_shape=pltpu.HBM((length, channels), jnp.float32),
        compiler_params=params(12),
        cost_estimate=cost(work),
        name="last",
    )(states, gains, powers, sent, before)


def solution(mesh):
    placed = (P("tm", "chan"), P(None, "chan"), P("chan"), P("tm"))

    def program(random_forcing, eigen_root_table, lane_fading_speed, sudden_shrink):
        length = random_forcing.shape[0] // mesh.shape["tm"]
        constants = tuple(jnp.asarray(table) for table in tables(length))

        def body(*args):
            return shards(args[:-4], *args[-4:])

        return jax.shard_map(
            body, mesh=mesh, in_specs=(P(None, None),) * len(constants) + placed,
            out_specs=P("tm", "chan"), check_vma=False,
        )(*constants, random_forcing, eigen_root_table, lane_fading_speed, sudden_shrink)

    return program
```

```python
import functools

import jax
import jax.numpy as jnp
import numpy as np
from jax import lax
from jax.experimental import pallas as pl
from jax.experimental.pallas import tpu as pltpu
from jax.sharding import PartitionSpec as P

LANES = 128
SEGMENTS = 8
BLOCK = 512
NYQUIST_ROWS = 16
OUT_BLOCK = 1024


def split(table):
    high = table.astype(jnp.bfloat16)
    low = (table - high.astype(np.float64)).astype(jnp.bfloat16)
    return high, low


def tripled(table):
    high, low = split(table)
    return np.concatenate([high, high, low], axis=1)


def tables(length):
    full = 2 * length
    half = length // 2
    frequency = 2 * np.arange(half)[:, None]
    nyquist = np.full((1, 1), length)

    def angle(frequencies, times):
        return (frequencies * times[None, :] % full) * (2.0 * np.pi / full)

    def parts(times):
        blank = np.zeros((NYQUIST_ROWS - 1, times.size))
        return (
            np.concatenate([np.cos(angle(frequency, times)), np.cos(angle(nyquist, times)), blank]),
            np.sin(angle(frequency, times)),
            np.cos(angle(frequency + 1, times)),
            np.sin(angle(frequency + 1, times)),
        )

    forward = np.concatenate(split(np.concatenate(parts(np.arange(length)))), axis=1)
    ticks = np.arange(length)
    counted = np.where(ticks < half, ticks, length - 1 - ticks)
    segment = half // SEGMENTS
    times = (np.arange(segment + 1)[:, None] + segment * np.arange(SEGMENTS)[None, :]).reshape(-1)
    even_cos, even_sin, odd_cos, odd_sin = (tripled(part.T / full) for part in parts(times))
    rows = counted // segment == np.arange(SEGMENTS)[:, None]
    blocks = counted % segment + np.where(ticks < half, 0, segment)
    blocks = blocks[:, None] == np.arange(2 * segment)
    return (
        forward, even_cos, even_sin, odd_cos, odd_sin,
        rows.astype(np.float32), blocks.astype(np.float32),
    )


def dot(left, right):
    return jnp.dot(left, right, preferred_element_type=jnp.float32)


def stacked(values):
    high = values.astype(jnp.bfloat16)
    low = (values - high.astype(jnp.float32)).astype(jnp.bfloat16)
    return jnp.concatenate([high, low, high], axis=0)


def spectra(section, evens, nyquist, odds, forward_ref):
    half = section.shape[0] // 2
    doubled = jnp.concatenate([section, section], axis=0)
    first = half + NYQUIST_ROWS
    scale = jnp.concatenate(
        [evens, jnp.broadcast_to(nyquist, (NYQUIST_ROWS, evens.shape[1]))], axis=0
    )
    even_cos = stacked(dot(forward_ref[:first], doubled) * scale)
    starts = (first, first + half, first + 2 * half)
    even_sin, odd_cos, odd_sin = (
        stacked(dot(forward_ref[at : at + half], doubled) * scale)
        for at, scale in zip(starts, (evens, odds, odds))
    )
    return even_cos, even_sin, odd_cos, odd_sin


def turned(x):
    row = lax.broadcasted_iota(jnp.int32, x.shape, 0)
    return jnp.take_along_axis(x, SEGMENTS - 1 - row, axis=0, mode="promise_in_bounds")


def mirrored(table_ref):
    full = table_ref.shape[0]
    half = full // 4
    row = lax.broadcasted_iota(jnp.int32, (SEGMENTS, LANES), 0)
    evens, odds = [], []
    for block in range(half // SEGMENTS):
        near = 2 * SEGMENTS * block
        direct = table_ref[pl.ds(near, SEGMENTS, stride=2), :]
        if block == 0:
            mirror = turned(table_ref[pl.ds(full - 2 * SEGMENTS, SEGMENTS, stride=2), :])
            mirror = jnp.where(row == 0, 0.0, pltpu.roll(mirror, 1, 0))
        else:
            mirror = turned(table_ref[pl.ds(full - near - 14, SEGMENTS, stride=2), :])
        evens.append(direct + mirror)
        direct = table_ref[pl.ds(near + 1, SEGMENTS, stride=2), :]
        mirror = turned(table_ref[pl.ds(full - near - 15, SEGMENTS, stride=2), :])
        odds.append(-(direct + mirror))
    return (
        jnp.concatenate(evens, axis=0),
        jnp.concatenate(odds, axis=0),
        table_ref[pl.ds(2 * half, 1), :],
    )


def wide(column, columns):
    return jnp.concatenate([column] * (columns // LANES), axis=1)


def one_minus_exp(x):
    series = jnp.ones_like(x)
    for term in range(9, 1, -1):
        series = 1.0 - x * series * (1.0 / term)
    return jnp.where(x < 0.4, x * series, 1.0 - jnp.exp(-x))


def spread(burst_ref, rows_ref, blocks_ref, out_ref):
    placed = jnp.dot(
        rows_ref[...] * burst_ref[...].reshape(1, -1), blocks_ref[...],
        precision=lax.Precision.HIGHEST, preferred_element_type=jnp.float32,
    )
    for block in range(placed.shape[1]):
        out_ref[pl.ds(block * SEGMENTS, SEGMENTS), :] = jnp.broadcast_to(
            placed[:, block : block + 1], (SEGMENTS, LANES)
        )


def orders(blocks):
    return (
        (range(blocks // 2), range(SEGMENTS)),
        (range(blocks - 1, blocks // 2 - 1, -1), range(SEGMENTS - 1, -1, -1)),
    )


def rows_of(block):
    return pl.ds(block * SEGMENTS, SEGMENTS)


def columns_of(step):
    return pl.ds(pl.multiple_of(step * BLOCK, BLOCK), BLOCK)


def scan(series, factors_ref, keep, fresh, states_ref=None, store=None):
    columns = keep.shape[1]
    entering = jnp.zeros((1, columns), jnp.float32)
    for order, rows in orders(factors_ref.shape[0] // SEGMENTS):
        state = decay = None
        for block in order:
            burst = factors_ref[rows_of(block), :]
            power = burst * burst
            variance = wide(1.0 - power, columns) + wide(power, columns) * fresh
            kick = variance * lax.rsqrt(variance) * series(block)
            factor = wide(burst, columns) * keep
            state = kick if state is None else factor * state + kick
            decay = factor if decay is None else factor * decay
            if states_ref is not None:
                states_ref[rows_of(block), :] = state
        before = [None] * SEGMENTS
        for row in rows:
            before[row] = entering
            entering = decay[row : row + 1] * entering + state[row : row + 1]
        if states_ref is not None:
            value = jnp.concatenate(before, axis=0)
            for block in order:
                value = wide(factors_ref[rows_of(block), :], columns) * keep * value
                store(block, states_ref[rows_of(block), :] + value)
    return entering


def load_kernel(section_hbm, table_hbm, rate_hbm, burst_hbm, *refs):
    sources, refs = refs[:7], refs[7:]
    part_refs, refs = refs[:3], refs[3:]
    table_ref, factors_ref, powers_ref, gains_ref = refs[:4]
    targets, (rate_ref, burst_ref, semaphores) = refs[4:11], refs[11:]
    length, channels = section_hbm.shape
    starts = (0, part_refs[0].shape[1], channels - part_refs[2].shape[1])
    copies = [
        pltpu.make_async_copy(source, target, semaphores.at[place])
        for place, (source, target) in enumerate(
            [(burst_hbm, burst_ref), *zip(sources[:2], targets[:2]), (rate_hbm, rate_ref)]
            + [
                (section_hbm.at[:, pl.ds(start, part_ref.shape[1])], part_ref)
                for start, part_ref in zip(starts, part_refs)
            ]
            + [
                (table_hbm.at[:, pl.ds(group * LANES, LANES)], table_ref.at[group])
                for group in range(BLOCK // LANES)
            ]
            + list(zip(sources[2:], targets[2:]))
        )
    ]
    for copy in copies:
        copy.start()
    for copy in copies[:4]:
        copy.wait()
    rows_ref, blocks_ref = targets[:2]
    spread(burst_ref, rows_ref, blocks_ref, factors_ref)
    shape = (length, length)
    earlier = lax.broadcasted_iota(jnp.int32, shape, 1) <= lax.broadcasted_iota(jnp.int32, shape, 0)
    logs = jnp.where(earlier, jnp.log(burst_ref[...].reshape(1, -1)), 0.0)
    powers_ref[...] = jnp.broadcast_to(
        jnp.exp(jnp.sum(logs, axis=1, keepdims=True)), (length, LANES)
    )
    rate = rate_ref[...]
    keep = jnp.exp(-rate)
    gains_ref[pl.ds(0, 1), :] = keep
    gains_ref[pl.ds(1, 1), :] = one_minus_exp(2.0 * rate)
    total = jnp.sum(jnp.log(factors_ref[...]), axis=0, keepdims=True)
    gains_ref[pl.ds(2, 1), :] = jnp.exp(wide(total, rate.shape[1]) - length * rate)
    for copy in copies[4:]:
        copy.wait()


def own_kernel(section_hbm, table_hbm, part_ref, first_ref, factors_ref, gains_ref, forward_ref, *refs):
    own_tables, refs = refs[:4], refs[4:]
    series_ref, after_ref, scale_ref, ends_ref, sums_ref, differences_ref = refs[:6]
    section_ref, table_ref, section_semaphores, table_semaphores = refs[6:]
    even_cos_ref, even_sin_ref, odd_cos_ref, odd_sin_ref = own_tables
    step = pl.program_id(0)
    length, channels = section_ref.shape
    half = length // 2
    segment = half // SEGMENTS
    groups = BLOCK // LANES

    def load_section(block):
        return pltpu.make_async_copy(
            section_hbm.at[:, columns_of(block)], section_ref.at[:, columns_of(block)],
            section_semaphores.at[block],
        )

    def load_table(group):
        columns = pl.ds(pl.multiple_of(group * LANES, LANES), LANES)
        return pltpu.make_async_copy(
            table_hbm.at[:, columns], table_ref.at[group], table_semaphores.at[group]
        )

    @pl.when(step == 0)
    def _():
        for block in range(1, channels // BLOCK):
            load_section(block).start()
            for group in range(groups):
                load_table(block * groups + group).start()
        section_ref[:, :BLOCK] = part_ref[:, :BLOCK]
        for group in range(groups):
            table_ref[group] = first_ref[group]

    @pl.when(step == pl.num_programs(0) - 1)
    def _():
        for target, first, second in (
            (sums_ref, even_cos_ref, odd_sin_ref), (differences_ref, even_sin_ref, odd_cos_ref)
        ):
            target[:, : first.shape[1]] = first[...]
            target[:, first.shape[1] :] = second[...]

    @pl.when(step > 0)
    def _():
        load_section(step).wait()
        for group in range(groups):
            load_table(step * groups + group).wait()

    for block in (step,):
        series, after, scale = (x.at[block] for x in (series_ref, after_ref, scale_ref))
        at = columns_of(block)
        evens, odds, nyquist = (
            jnp.concatenate(part, axis=1)
            for part in zip(
                *(mirrored(table_ref.at[block * groups + group]) for group in range(groups))
            )
        )
        scale[pl.ds(0, half), :] = evens
        scale[pl.ds(half, half), :] = odds
        scale[pl.ds(length, SEGMENTS), :] = jnp.broadcast_to(nyquist, (SEGMENTS, BLOCK))
        even_cos, even_sin, odd_cos, odd_sin = (
            dot(inverse_ref[...], part)
            for inverse_ref, part in zip(
                own_tables, spectra(section_ref[:, at], evens, nyquist, odds, forward_ref)
            )
        )
        for row in range(segment + 1):
            rows = slice(row * SEGMENTS, (row + 1) * SEGMENTS)
            ec, es, oc, os = even_cos[rows], even_sin[rows], odd_cos[rows], odd_sin[rows]
            if row < segment:
                even, odd = ec + es, oc + os
                series[rows_of(row), :] = even - odd
                after[rows_of(row), :] = even + odd
            if row > 0:
                even, odd = ec - es, os - oc
                series[rows_of(segment + row - 1), :] = even - odd
                after[rows_of(segment + row - 1), :] = even + odd
        ends_ref[pl.ds(0, 1), at] = scan(
            lambda row: series[rows_of(row), :], factors_ref,
            gains_ref[pl.ds(0, 1), at], gains_ref[pl.ds(1, 1), at],
        )


def next_kernel(after_ref, ends_ref, gains_ref, burst_ref, rows_ref, blocks_ref, out_ref, factors_ref):
    step = pl.program_id(0)

    @pl.when(step == 0)
    def _():
        spread(burst_ref, rows_ref, blocks_ref, factors_ref)

    after_ref = after_ref.at[step]
    columns = after_ref.shape[1]
    at = columns_of(step)
    out_ref[pl.ds(0, 1), at] = ends_ref[pl.ds(0, 1), at]
    out_ref[pl.ds(1, 1), at] = scan(
        lambda block: after_ref[rows_of(block), :], factors_ref,
        gains_ref[pl.ds(0, 1), at], gains_ref[pl.ds(1, 1), at],
    )
    out_ref[pl.ds(2, 1), at] = gains_ref[pl.ds(2, 1), at]
    out_ref[pl.ds(3, 1), at] = jnp.ones((1, columns), jnp.float32)


def merge_kernel(step, sent_ref, got_ref, *refs):
    *before_ref, out_ref, after_ref = refs
    later = (lax.axis_index("tm") // step) % 2 == 1
    sent, got = sent_ref[...], got_ref[...]
    low = jnp.where(later, got, sent)
    high = jnp.where(later, sent, got)
    out_ref[pl.ds(0, 1), :] = high[:1] + high[2:3] * low[:1] + high[3:] * low[1:2]
    out_ref[pl.ds(1, 1), :] = high[1:2]
    out_ref[pl.ds(2, 1), :] = high[2:3] * low[2:3]
    out_ref[pl.ds(3, 1), :] = high[2:3] * low[3:]
    if before_ref:
        before, decay, decay_later = (before_ref[0][pl.ds(row, 1), :] for row in range(3))
    else:
        decay = jnp.ones_like(sent[:1])
        before = decay_later = jnp.zeros_like(decay)
    added = before + decay * got[:1] + decay_later * got[1:2]
    after_ref[pl.ds(0, 1), :] = jnp.where(later, added, before)
    after_ref[pl.ds(1, 1), :] = jnp.where(later, decay * got[2:3], decay)
    after_ref[pl.ds(2, 1), :] = jnp.where(later, decay * got[3:], decay_later)


def middle_kernel(
    first, begin, section_ref, gains_ref, scale_ref, series_ref, factors_ref, forward_ref, sums_ref,
    differences_ref, *refs,
):
    *_, states_ref, work_ref = refs
    step = first + pl.program_id(0)
    at_columns = columns_of(step)
    scale_ref, series_ref = scale_ref.at[step], series_ref.at[step]
    length = section_ref.shape[0]
    half = length // 2
    segment = half // SEGMENTS
    even_cos, even_sin, odd_cos, odd_sin = spectra(
        section_ref[:, columns_of(step - begin)],
        scale_ref[pl.ds(0, half), :],
        scale_ref[pl.ds(length, 1), :],
        scale_ref[pl.ds(half, half), :],
        forward_ref,
    )
    sums = dot(sums_ref[...], jnp.concatenate([even_cos, odd_sin], axis=0))
    differences = dot(differences_ref[...], jnp.concatenate([even_sin, odd_cos], axis=0))
    for block in range(segment + 1):
        at = slice(block * SEGMENTS, (block + 1) * SEGMENTS)
        if block < segment:
            place = rows_of(block)
            work_ref[place, :] = sums[at] + differences[at] + series_ref[place, :]
        if block > 0:
            place = rows_of(segment + block - 1)
            work_ref[place, :] = sums[at] - differences[at] + series_ref[place, :]
    groups = BLOCK // LANES

    def store(block, value):
        if block < segment:
            start = block
        else:
            value = turned(value)
            start = length - 1 - (block - segment) - (SEGMENTS - 1) * segment
        for group in range(groups):
            states_ref[step * groups + group, pl.ds(start, SEGMENTS, stride=segment), :] = value[
                :, group * LANES : (group + 1) * LANES
            ]

    scan(
        lambda block: work_ref[rows_of(block), :], factors_ref,
        gains_ref[pl.ds(0, 1), at_columns], gains_ref[pl.ds(1, 1), at_columns], work_ref, store,
    )


def last_kernel(states_ref, gains_ref, powers_ref, sent_ref, before_ref, out_ref):
    step = pl.program_id(0)
    length, columns = out_ref.shape
    at = pl.ds(pl.multiple_of(step * columns, columns), columns)
    keep = gains_ref[pl.ds(0, 1), at]
    state, spill, total, later = (sent_ref[pl.ds(row, 1), at] for row in range(4))
    before, decay, decay_later = (before_ref[pl.ds(row, 1), at] for row in range(3))
    opening = (state + later * spill) / (1.0 - total)
    entering = before + decay * opening + decay_later * spill
    rows = []
    for _ in range(SEGMENTS):
        entering = keep * entering
        rows.append(entering)
    value = jnp.concatenate(rows, axis=0)
    jump = keep
    for _ in range(SEGMENTS.bit_length() - 1):
        jump = jump * jump
    groups = columns // LANES
    for block in range(length // SEGMENTS):
        place = rows_of(block)
        states = jnp.concatenate(
            [states_ref[step * groups + group, place, :] for group in range(groups)], axis=1
        )
        out_ref[place, :] = states + wide(powers_ref[place, :], columns) * value
        value = jump * value


VMEM = pl.BlockSpec(memory_space=pltpu.VMEM)
HBM = pl.BlockSpec(memory_space=pltpu.HBM)


def in_hbm(array):
    return pltpu.with_memory_space_constraint(array, pltpu.HBM)


def cost(flops):
    return pl.CostEstimate(flops=flops, bytes_accessed=2**24, transcendentals=0)


def params(mebibytes):
    return pltpu.CompilerParams(vmem_limit_bytes=mebibytes * 2**20)


def shards(constants, random_forcing, eigen_root_table, lane_fading_speed, sudden_shrink):
    tables, (rows, places) = constants[:5], constants[5:]
    length, channels = random_forcing.shape
    count = lax.axis_size("tm")
    steps = channels // BLOCK
    ahead = [(i, (i + 1) % count) for i in range(count)]
    back = [((i + 1) % count, i) for i in range(count)]
    rate = lane_fading_speed[None, :]
    work = 2 * channels * length * length

    def vmem(*shape, dtype=jnp.float32):
        return pltpu.VMEM(shape, dtype)

    def kept(table):
        return vmem(*table.shape, dtype=table.dtype)

    def joined(pair):
        return vmem(
            pair[0].shape[0], sum(table.shape[1] for table in pair), dtype=pair[0].dtype
        )

    cuts = (0, steps // 2, steps - max(1, steps // 4), steps)
    loaded = pl.pallas_call(
        load_kernel,
        in_specs=[HBM] * 11,
        out_specs=[VMEM] * 14,
        out_shape=[
            *(
                vmem(length, width * BLOCK, dtype=random_forcing.dtype)
                for width in (end - start for start, end in zip(cuts, cuts[1:]))
            ),
            vmem(BLOCK // LANES, 2 * length, LANES), vmem(length, LANES), vmem(length, LANES),
            vmem(SEGMENTS, channels), *map(kept, (rows, places, *tables)),
        ],
        scratch_shapes=[vmem(1, channels), vmem(length), pltpu.SemaphoreType.DMA((16,))],
        compiler_params=params(8),
        cost_estimate=cost(work // 4),
        name="load",
    )(*map(in_hbm, (random_forcing, eigen_root_table, rate, sudden_shrink, rows, places, *tables)))

    parts, inverses = loaded[:3], loaded[10:]
    first, factors, powers, gains, rows, places, forward = loaded[3:10]
    previous = []
    for part in range(3):
        previous.append(lax.ppermute(parts[part], "tm", ahead))
    following = lax.ppermute(sudden_shrink, "tm", back)

    series, after, scale, ends, *middle_tables = pl.pallas_call(
        own_kernel,
        grid=(steps,),
        in_specs=[HBM] * 2 + [VMEM] * 9,
        out_specs=[VMEM] * 6,
        out_shape=[
            vmem(steps, length, BLOCK), vmem(steps, length, BLOCK),
            vmem(steps, length + SEGMENTS, BLOCK), vmem(1, channels),
            *map(joined, (inverses[::3], inverses[1:3])),
        ],
        scratch_shapes=[
            kept(random_forcing), vmem(channels // LANES, 2 * length, LANES),
            pltpu.SemaphoreType.DMA((steps,)), pltpu.SemaphoreType.DMA((channels // LANES,)),
        ],
        compiler_params=params(22),
        cost_estimate=cost(7 * work),
        name="own",
    )(
        in_hbm(random_forcing), in_hbm(eigen_root_table), parts[0], first, factors, gains,
        forward, *inverses,
    )

    sent = pl.pallas_call(
        next_kernel,
        grid=(steps,),
        in_specs=[VMEM] * 6,
        out_specs=VMEM,
        out_shape=vmem(4, channels),
        scratch_shapes=[vmem(length, LANES)],
        compiler_params=params(16),
        cost_estimate=cost(work),
        name="next",
    )(after, ends, gains, following, rows, places)

    states = ()
    pieces = (
        (0, cuts[1] // 2, 0, 0), (cuts[1] // 2, cuts[1], 0, 0),
        (cuts[1], cuts[2], 1, cuts[1]), (cuts[2], cuts[3], 2, cuts[2]),
    )
    for first, end, source, begin in pieces:
        states = (
            pl.pallas_call(
                functools.partial(middle_kernel, first, begin),
                grid=(end - first,),
                in_specs=[VMEM] * (8 + len(states)),
                out_specs=VMEM,
                out_shape=vmem(channels // LANES, length, LANES),
                scratch_shapes=[vmem(length, BLOCK)],
                input_output_aliases={8: 0} if states else {},
                compiler_params=params(24),
                cost_estimate=cost(4 * work),
                name="middle",
            )(previous[source], gains, scale, series, factors, forward, *middle_tables, *states),
        )
    (states,) = states

    before = None
    step = 1
    while step < count:
        got = lax.ppermute(sent, "tm", [(i, i ^ step) for i in range(count)])
        kept_rows = () if before is None else (before,)
        sent, before = pl.pallas_call(
            functools.partial(merge_kernel, step),
            in_specs=[VMEM] * (2 + len(kept_rows)),
            out_specs=[VMEM] * 2,
            out_shape=[vmem(4, channels), vmem(3, channels)],
            compiler_params=params(4),
            cost_estimate=cost(channels),
            name="merge",
        )(sent, got, *kept_rows)
        step *= 2

    return pl.pallas_call(
        last_kernel,
        grid=(channels // OUT_BLOCK,),
        in_specs=[VMEM] * 5,
        out_specs=pl.BlockSpec((length, OUT_BLOCK), lambda i: (0, i)),
        out_shape=pltpu.HBM((length, channels), jnp.float32),
        compiler_params=params(12),
        cost_estimate=cost(work),
        name="last",
    )(states, gains, powers, sent, before)


def solution(mesh):
    placed = (P("tm", "chan"), P(None, "chan"), P("chan"), P("tm"))

    def program(random_forcing, eigen_root_table, lane_fading_speed, sudden_shrink):
        length = random_forcing.shape[0] // mesh.shape["tm"]
        constants = tuple(jnp.asarray(table) for table in tables(length))

        def body(*args):
            return shards(args[:-4], *args[-4:])

        return jax.shard_map(
            body, mesh=mesh, in_specs=(P(None, None),) * len(constants) + placed,
            out_specs=P("tm", "chan"), check_vma=False,
        )(*constants, random_forcing, eigen_root_table, lane_fading_speed, sudden_shrink)

    return program
```

```python
import functools

import jax
import jax.numpy as jnp
import numpy as np
from jax import lax
from jax.experimental import pallas as pl
from jax.experimental.pallas import tpu as pltpu
from jax.sharding import PartitionSpec as P

LANES = 128
SEGMENTS = 8
BLOCK = 512
NYQUIST_ROWS = 16
OUT_BLOCK = 1024


def split(table):
    high = table.astype(jnp.bfloat16)
    low = (table - high.astype(np.float64)).astype(jnp.bfloat16)
    return high, low


def tripled(table):
    high, low = split(table)
    return np.concatenate([high, high, low], axis=1)


def tables(length):
    full = 2 * length
    half = length // 2
    frequency = 2 * np.arange(half)[:, None]
    nyquist = np.full((1, 1), length)

    def angle(frequencies, times):
        return (frequencies * times[None, :] % full) * (2.0 * np.pi / full)

    def parts(times):
        blank = np.zeros((NYQUIST_ROWS - 1, times.size))
        return (
            np.concatenate([np.cos(angle(frequency, times)), np.cos(angle(nyquist, times)), blank]),
            np.sin(angle(frequency, times)),
            np.cos(angle(frequency + 1, times)),
            np.sin(angle(frequency + 1, times)),
        )

    forward = np.concatenate(split(np.concatenate(parts(np.arange(length)))), axis=1)
    ticks = np.arange(length)
    counted = np.where(ticks < half, ticks, length - 1 - ticks)
    segment = half // SEGMENTS
    times = (np.arange(segment + 1)[:, None] + segment * np.arange(SEGMENTS)[None, :]).reshape(-1)
    even_cos, even_sin, odd_cos, odd_sin = (tripled(part.T / full) for part in parts(times))
    rows = counted // segment == np.arange(SEGMENTS)[:, None]
    blocks = counted % segment + np.where(ticks < half, 0, segment)
    blocks = blocks[:, None] == np.arange(2 * segment)
    return (
        forward, even_cos, even_sin, odd_cos, odd_sin,
        rows.astype(np.float32), blocks.astype(np.float32),
    )


def dot(left, right):
    return jnp.dot(left, right, preferred_element_type=jnp.float32)


def stacked(values):
    high = values.astype(jnp.bfloat16)
    low = (values - high.astype(jnp.float32)).astype(jnp.bfloat16)
    return jnp.concatenate([high, low, high], axis=0)


def spectra(section, evens, nyquist, odds, forward_ref):
    half = section.shape[0] // 2
    doubled = jnp.concatenate([section, section], axis=0)
    first = half + NYQUIST_ROWS
    scale = jnp.concatenate(
        [evens, jnp.broadcast_to(nyquist, (NYQUIST_ROWS, evens.shape[1]))], axis=0
    )
    even_cos = stacked(dot(forward_ref[:first], doubled) * scale)
    starts = (first, first + half, first + 2 * half)
    even_sin, odd_cos, odd_sin = (
        stacked(dot(forward_ref[at : at + half], doubled) * scale)
        for at, scale in zip(starts, (evens, odds, odds))
    )
    return even_cos, even_sin, odd_cos, odd_sin


def turned(x):
    row = lax.broadcasted_iota(jnp.int32, x.shape, 0)
    return jnp.take_along_axis(x, SEGMENTS - 1 - row, axis=0, mode="promise_in_bounds")


def mirrored(table_ref):
    full = table_ref.shape[0]
    half = full // 4
    row = lax.broadcasted_iota(jnp.int32, (SEGMENTS, LANES), 0)
    evens, odds = [], []
    for block in range(half // SEGMENTS):
        near = 2 * SEGMENTS * block
        direct = table_ref[pl.ds(near, SEGMENTS, stride=2), :]
        if block == 0:
            mirror = turned(table_ref[pl.ds(full - 2 * SEGMENTS, SEGMENTS, stride=2), :])
            mirror = jnp.where(row == 0, 0.0, pltpu.roll(mirror, 1, 0))
        else:
            mirror = turned(table_ref[pl.ds(full - near - 14, SEGMENTS, stride=2), :])
        evens.append(direct + mirror)
        direct = table_ref[pl.ds(near + 1, SEGMENTS, stride=2), :]
        mirror = turned(table_ref[pl.ds(full - near - 15, SEGMENTS, stride=2), :])
        odds.append(-(direct + mirror))
    return (
        jnp.concatenate(evens, axis=0),
        jnp.concatenate(odds, axis=0),
        table_ref[pl.ds(2 * half, 1), :],
    )


def wide(column, columns):
    return jnp.concatenate([column] * (columns // LANES), axis=1)


def one_minus_exp(x):
    series = jnp.ones_like(x)
    for term in range(9, 1, -1):
        series = 1.0 - x * series * (1.0 / term)
    return jnp.where(x < 0.4, x * series, 1.0 - jnp.exp(-x))


def spread(burst_ref, rows_ref, blocks_ref, out_ref):
    placed = jnp.dot(
        rows_ref[...] * burst_ref[...].reshape(1, -1), blocks_ref[...],
        precision=lax.Precision.HIGHEST, preferred_element_type=jnp.float32,
    )
    for block in range(placed.shape[1]):
        out_ref[pl.ds(block * SEGMENTS, SEGMENTS), :] = jnp.broadcast_to(
            placed[:, block : block + 1], (SEGMENTS, LANES)
        )


def orders(blocks):
    return (
        (range(blocks // 2), range(SEGMENTS)),
        (range(blocks - 1, blocks // 2 - 1, -1), range(SEGMENTS - 1, -1, -1)),
    )


def rows_of(block):
    return pl.ds(block * SEGMENTS, SEGMENTS)


def columns_of(step):
    return pl.ds(pl.multiple_of(step * BLOCK, BLOCK), BLOCK)


def scan(series, factors_ref, keep, fresh, states_ref=None, store=None):
    columns = keep.shape[1]
    entering = jnp.zeros((1, columns), jnp.float32)
    for order, rows in orders(factors_ref.shape[0] // SEGMENTS):
        state = decay = None
        for block in order:
            burst = factors_ref[rows_of(block), :]
            power = burst * burst
            variance = wide(1.0 - power, columns) + wide(power, columns) * fresh
            kick = variance * lax.rsqrt(variance) * series(block)
            factor = wide(burst, columns) * keep
            state = kick if state is None else factor * state + kick
            decay = factor if decay is None else factor * decay
            if states_ref is not None:
                states_ref[rows_of(block), :] = state
        before = [None] * SEGMENTS
        for row in rows:
            before[row] = entering
            entering = decay[row : row + 1] * entering + state[row : row + 1]
        if states_ref is not None:
            value = jnp.concatenate(before, axis=0)
            for block in order:
                value = wide(factors_ref[rows_of(block), :], columns) * keep * value
                store(block, states_ref[rows_of(block), :] + value)
    return entering


def load_kernel(section_hbm, table_hbm, rate_hbm, burst_hbm, *refs):
    sources, refs = refs[:7], refs[7:]
    part_refs, refs = refs[:3], refs[3:]
    table_ref, factors_ref, powers_ref, gains_ref = refs[:4]
    targets, (rate_ref, burst_ref, semaphores) = refs[4:11], refs[11:]
    length, channels = section_hbm.shape
    starts = (0, part_refs[0].shape[1], channels - part_refs[2].shape[1])
    copies = [
        pltpu.make_async_copy(source, target, semaphores.at[place])
        for place, (source, target) in enumerate(
            [(burst_hbm, burst_ref), *zip(sources[:2], targets[:2]), (rate_hbm, rate_ref)]
            + [
                (section_hbm.at[:, pl.ds(start, part_ref.shape[1])], part_ref)
                for start, part_ref in zip(starts, part_refs)
            ]
            + [
                (table_hbm.at[:, pl.ds(group * LANES, LANES)], table_ref.at[group])
                for group in range(BLOCK // LANES)
            ]
            + list(zip(sources[2:], targets[2:]))
        )
    ]
    for copy in copies:
        copy.start()
    for copy in copies[:4]:
        copy.wait()
    rows_ref, blocks_ref = targets[:2]
    spread(burst_ref, rows_ref, blocks_ref, factors_ref)
    shape = (length, length)
    earlier = lax.broadcasted_iota(jnp.int32, shape, 1) <= lax.broadcasted_iota(jnp.int32, shape, 0)
    logs = jnp.where(earlier, jnp.log(burst_ref[...].reshape(1, -1)), 0.0)
    powers_ref[...] = jnp.broadcast_to(
        jnp.exp(jnp.sum(logs, axis=1, keepdims=True)), (length, LANES)
    )
    rate = rate_ref[...]
    keep = jnp.exp(-rate)
    gains_ref[pl.ds(0, 1), :] = keep
    gains_ref[pl.ds(1, 1), :] = one_minus_exp(2.0 * rate)
    total = jnp.sum(jnp.log(factors_ref[...]), axis=0, keepdims=True)
    gains_ref[pl.ds(2, 1), :] = jnp.exp(wide(total, rate.shape[1]) - length * rate)
    for copy in copies[4:]:
        copy.wait()


def own_kernel(section_hbm, table_hbm, part_ref, first_ref, factors_ref, gains_ref, forward_ref, *refs):
    own_tables, refs = refs[:4], refs[4:]
    series_ref, after_ref, scale_ref, ends_ref, sums_ref, differences_ref = refs[:6]
    section_ref, table_ref, section_semaphores, table_semaphores = refs[6:]
    even_cos_ref, even_sin_ref, odd_cos_ref, odd_sin_ref = own_tables
    step = pl.program_id(0)
    length, channels = section_ref.shape
    half = length // 2
    segment = half // SEGMENTS
    groups = BLOCK // LANES

    def load_section(block):
        return pltpu.make_async_copy(
            section_hbm.at[:, columns_of(block)], section_ref.at[:, columns_of(block)],
            section_semaphores.at[block],
        )

    def load_table(group):
        columns = pl.ds(pl.multiple_of(group * LANES, LANES), LANES)
        return pltpu.make_async_copy(
            table_hbm.at[:, columns], table_ref.at[group], table_semaphores.at[group]
        )

    @pl.when(step == 0)
    def _():
        for block in range(1, channels // BLOCK):
            load_section(block).start()
            for group in range(groups):
                load_table(block * groups + group).start()
        section_ref[:, :BLOCK] = part_ref[:, :BLOCK]
        for group in range(groups):
            table_ref[group] = first_ref[group]

    @pl.when(step == pl.num_programs(0) - 1)
    def _():
        for target, first, second in (
            (sums_ref, even_cos_ref, odd_sin_ref), (differences_ref, even_sin_ref, odd_cos_ref)
        ):
            target[:, : first.shape[1]] = first[...]
            target[:, first.shape[1] :] = second[...]

    @pl.when(step > 0)
    def _():
        load_section(step).wait()
        for group in range(groups):
            load_table(step * groups + group).wait()

    for block in (step,):
        series, after, scale = (x.at[block] for x in (series_ref, after_ref, scale_ref))
        at = columns_of(block)
        evens, odds, nyquist = (
            jnp.concatenate(part, axis=1)
            for part in zip(
                *(mirrored(table_ref.at[block * groups + group]) for group in range(groups))
            )
        )
        scale[pl.ds(0, half), :] = evens
        scale[pl.ds(half, half), :] = odds
        scale[pl.ds(length, SEGMENTS), :] = jnp.broadcast_to(nyquist, (SEGMENTS, BLOCK))
        even_cos, even_sin, odd_cos, odd_sin = (
            dot(inverse_ref[...], part)
            for inverse_ref, part in zip(
                own_tables, spectra(section_ref[:, at], evens, nyquist, odds, forward_ref)
            )
        )
        for row in range(segment + 1):
            rows = slice(row * SEGMENTS, (row + 1) * SEGMENTS)
            ec, es, oc, os = even_cos[rows], even_sin[rows], odd_cos[rows], odd_sin[rows]
            if row < segment:
                even, odd = ec + es, oc + os
                series[rows_of(row), :] = even - odd
                after[rows_of(row), :] = even + odd
            if row > 0:
                even, odd = ec - es, os - oc
                series[rows_of(segment + row - 1), :] = even - odd
                after[rows_of(segment + row - 1), :] = even + odd
        ends_ref[pl.ds(0, 1), at] = scan(
            lambda row: series[rows_of(row), :], factors_ref,
            gains_ref[pl.ds(0, 1), at], gains_ref[pl.ds(1, 1), at],
        )


def next_kernel(after_ref, ends_ref, gains_ref, burst_ref, rows_ref, blocks_ref, out_ref, factors_ref):
    step = pl.program_id(0)

    @pl.when(step == 0)
    def _():
        spread(burst_ref, rows_ref, blocks_ref, factors_ref)

    for block in (2 * step, 2 * step + 1):
        after, at = after_ref.at[block], columns_of(block)
        out_ref[pl.ds(0, 1), at] = ends_ref[pl.ds(0, 1), at]
        out_ref[pl.ds(1, 1), at] = scan(
            lambda row, after=after: after[rows_of(row), :], factors_ref,
            gains_ref[pl.ds(0, 1), at], gains_ref[pl.ds(1, 1), at],
        )
        out_ref[pl.ds(2, 1), at] = gains_ref[pl.ds(2, 1), at]
        out_ref[pl.ds(3, 1), at] = jnp.ones((1, BLOCK), jnp.float32)


def merge_kernel(step, sent_ref, got_ref, *refs):
    *before_ref, out_ref, after_ref = refs
    later = (lax.axis_index("tm") // step) % 2 == 1
    sent, got = sent_ref[...], got_ref[...]
    low = jnp.where(later, got, sent)
    high = jnp.where(later, sent, got)
    out_ref[pl.ds(0, 1), :] = high[:1] + high[2:3] * low[:1] + high[3:] * low[1:2]
    out_ref[pl.ds(1, 1), :] = high[1:2]
    out_ref[pl.ds(2, 1), :] = high[2:3] * low[2:3]
    out_ref[pl.ds(3, 1), :] = high[2:3] * low[3:]
    if before_ref:
        before, decay, decay_later = (before_ref[0][pl.ds(row, 1), :] for row in range(3))
    else:
        decay = jnp.ones_like(sent[:1])
        before = decay_later = jnp.zeros_like(decay)
    added = before + decay * got[:1] + decay_later * got[1:2]
    after_ref[pl.ds(0, 1), :] = jnp.where(later, added, before)
    after_ref[pl.ds(1, 1), :] = jnp.where(later, decay * got[2:3], decay)
    after_ref[pl.ds(2, 1), :] = jnp.where(later, decay * got[3:], decay_later)


def middle_kernel(
    first, begin, section_ref, gains_ref, scale_ref, series_ref, factors_ref, forward_ref, sums_ref,
    differences_ref, *refs,
):
    *_, states_ref, work_ref = refs
    step = first + pl.program_id(0)
    at_columns = columns_of(step)
    scale_ref, series_ref = scale_ref.at[step], series_ref.at[step]
    length = section_ref.shape[0]
    half = length // 2
    segment = half // SEGMENTS
    even_cos, even_sin, odd_cos, odd_sin = spectra(
        section_ref[:, columns_of(step - begin)],
        scale_ref[pl.ds(0, half), :],
        scale_ref[pl.ds(length, 1), :],
        scale_ref[pl.ds(half, half), :],
        forward_ref,
    )
    sums = dot(sums_ref[...], jnp.concatenate([even_cos, odd_sin], axis=0))
    differences = dot(differences_ref[...], jnp.concatenate([even_sin, odd_cos], axis=0))
    for block in range(segment + 1):
        at = slice(block * SEGMENTS, (block + 1) * SEGMENTS)
        if block < segment:
            place = rows_of(block)
            work_ref[place, :] = sums[at] + differences[at] + series_ref[place, :]
        if block > 0:
            place = rows_of(segment + block - 1)
            work_ref[place, :] = sums[at] - differences[at] + series_ref[place, :]
    groups = BLOCK // LANES

    def store(block, value):
        if block < segment:
            start = block
        else:
            value = turned(value)
            start = length - 1 - (block - segment) - (SEGMENTS - 1) * segment
        for group in range(groups):
            states_ref[step * groups + group, pl.ds(start, SEGMENTS, stride=segment), :] = value[
                :, group * LANES : (group + 1) * LANES
            ]

    scan(
        lambda block: work_ref[rows_of(block), :], factors_ref,
        gains_ref[pl.ds(0, 1), at_columns], gains_ref[pl.ds(1, 1), at_columns], work_ref, store,
    )


def last_kernel(states_ref, gains_ref, powers_ref, sent_ref, before_ref, out_ref):
    step = pl.program_id(0)
    length, columns = out_ref.shape
    at = pl.ds(pl.multiple_of(step * columns, columns), columns)
    keep = gains_ref[pl.ds(0, 1), at]
    state, spill, total, later = (sent_ref[pl.ds(row, 1), at] for row in range(4))
    before, decay, decay_later = (before_ref[pl.ds(row, 1), at] for row in range(3))
    opening = (state + later * spill) / (1.0 - total)
    entering = before + decay * opening + decay_later * spill
    rows = []
    for _ in range(SEGMENTS):
        entering = keep * entering
        rows.append(entering)
    value = jnp.concatenate(rows, axis=0)
    jump = keep
    for _ in range(SEGMENTS.bit_length() - 1):
        jump = jump * jump
    groups = columns // LANES
    for block in range(length // SEGMENTS):
        place = rows_of(block)
        states = jnp.concatenate(
            [states_ref[step * groups + group, place, :] for group in range(groups)], axis=1
        )
        out_ref[place, :] = states + wide(powers_ref[place, :], columns) * value
        value = jump * value


VMEM = pl.BlockSpec(memory_space=pltpu.VMEM)
HBM = pl.BlockSpec(memory_space=pltpu.HBM)


def in_hbm(array):
    return pltpu.with_memory_space_constraint(array, pltpu.HBM)


def cost(flops):
    return pl.CostEstimate(flops=flops, bytes_accessed=2**24, transcendentals=0)


def params(mebibytes):
    return pltpu.CompilerParams(vmem_limit_bytes=mebibytes * 2**20)


def shards(constants, random_forcing, eigen_root_table, lane_fading_speed, sudden_shrink):
    tables, (rows, places) = constants[:5], constants[5:]
    length, channels = random_forcing.shape
    count = lax.axis_size("tm")
    steps = channels // BLOCK
    ahead = [(i, (i + 1) % count) for i in range(count)]
    back = [((i + 1) % count, i) for i in range(count)]
    rate = lane_fading_speed[None, :]
    work = 2 * channels * length * length

    def vmem(*shape, dtype=jnp.float32):
        return pltpu.VMEM(shape, dtype)

    def kept(table):
        return vmem(*table.shape, dtype=table.dtype)

    def joined(pair):
        return vmem(
            pair[0].shape[0], sum(table.shape[1] for table in pair), dtype=pair[0].dtype
        )

    cuts = (0, steps // 2, steps - max(1, steps // 4), steps)
    loaded = pl.pallas_call(
        load_kernel,
        in_specs=[HBM] * 11,
        out_specs=[VMEM] * 14,
        out_shape=[
            *(
                vmem(length, width * BLOCK, dtype=random_forcing.dtype)
                for width in (end - start for start, end in zip(cuts, cuts[1:]))
            ),
            vmem(BLOCK // LANES, 2 * length, LANES), vmem(length, LANES), vmem(length, LANES),
            vmem(SEGMENTS, channels), *map(kept, (rows, places, *tables)),
        ],
        scratch_shapes=[vmem(1, channels), vmem(length), pltpu.SemaphoreType.DMA((16,))],
        compiler_params=params(8),
        cost_estimate=cost(work // 4),
        name="load",
    )(*map(in_hbm, (random_forcing, eigen_root_table, rate, sudden_shrink, rows, places, *tables)))

    parts, inverses = loaded[:3], loaded[10:]
    first, factors, powers, gains, rows, places, forward = loaded[3:10]
    previous = []
    for part in range(3):
        previous.append(lax.ppermute(parts[part], "tm", ahead))
    following = lax.ppermute(sudden_shrink, "tm", back)

    series, after, scale, ends, *middle_tables = pl.pallas_call(
        own_kernel,
        grid=(steps,),
        in_specs=[HBM] * 2 + [VMEM] * 9,
        out_specs=[VMEM] * 6,
        out_shape=[
            vmem(steps, length, BLOCK), vmem(steps, length, BLOCK),
            vmem(steps, length + SEGMENTS, BLOCK), vmem(1, channels),
            *map(joined, (inverses[::3], inverses[1:3])),
        ],
        scratch_shapes=[
            kept(random_forcing), vmem(channels // LANES, 2 * length, LANES),
            pltpu.SemaphoreType.DMA((steps,)), pltpu.SemaphoreType.DMA((channels // LANES,)),
        ],
        compiler_params=params(22),
        cost_estimate=cost(7 * work),
        name="own",
    )(
        in_hbm(random_forcing), in_hbm(eigen_root_table), parts[0], first, factors, gains,
        forward, *inverses,
    )

    sent = pl.pallas_call(
        next_kernel,
        grid=(steps // 2,),
        in_specs=[VMEM] * 6,
        out_specs=VMEM,
        out_shape=vmem(4, channels),
        scratch_shapes=[vmem(length, LANES)],
        compiler_params=params(16),
        cost_estimate=cost(work),
        name="next",
    )(after, ends, gains, following, rows, places)

    states = ()
    pieces = (
        (0, cuts[1] // 2, 0, 0), (cuts[1] // 2, cuts[1], 0, 0),
        (cuts[1], cuts[2], 1, cuts[1]), (cuts[2], cuts[3], 2, cuts[2]),
    )
    for first, end, source, begin in pieces:
        states = (
            pl.pallas_call(
                functools.partial(middle_kernel, first, begin),
                grid=(end - first,),
                in_specs=[VMEM] * (8 + len(states)),
                out_specs=VMEM,
                out_shape=vmem(channels // LANES, length, LANES),
                scratch_shapes=[vmem(length, BLOCK)],
                input_output_aliases={8: 0} if states else {},
                compiler_params=params(24),
                cost_estimate=cost(4 * work),
                name="middle",
            )(previous[source], gains, scale, series, factors, forward, *middle_tables, *states),
        )
    (states,) = states

    before = None
    step = 1
    while step < count:
        got = lax.ppermute(sent, "tm", [(i, i ^ step) for i in range(count)])
        kept_rows = () if before is None else (before,)
        sent, before = pl.pallas_call(
            functools.partial(merge_kernel, step),
            in_specs=[VMEM] * (2 + len(kept_rows)),
            out_specs=[VMEM] * 2,
            out_shape=[vmem(4, channels), vmem(3, channels)],
            compiler_params=params(4),
            cost_estimate=cost(channels),
            name="merge",
        )(sent, got, *kept_rows)
        step *= 2

    return pl.pallas_call(
        last_kernel,
        grid=(channels // OUT_BLOCK,),
        in_specs=[VMEM] * 5,
        out_specs=pl.BlockSpec((length, OUT_BLOCK), lambda i: (0, i)),
        out_shape=pltpu.HBM((length, channels), jnp.float32),
        compiler_params=params(12),
        cost_estimate=cost(work),
        name="last",
    )(states, gains, powers, sent, before)


def solution(mesh):
    placed = (P("tm", "chan"), P(None, "chan"), P("chan"), P("tm"))

    def program(random_forcing, eigen_root_table, lane_fading_speed, sudden_shrink):
        length = random_forcing.shape[0] // mesh.shape["tm"]
        constants = tuple(jnp.asarray(table) for table in tables(length))

        def body(*args):
            return shards(args[:-4], *args[-4:])

        return jax.shard_map(
            body, mesh=mesh, in_specs=(P(None, None),) * len(constants) + placed,
            out_specs=P("tm", "chan"), check_vma=False,
        )(*constants, random_forcing, eigen_root_table, lane_fading_speed, sudden_shrink)

    return program
```
